32 devices in a mesh: shot: 4 (over y, core), space: 8 (over z, x).
Axes of the slice: x: 2, y: 2, z: 4, core: 2. Of those that a mesh axis runs over, the one named last changes fastest.
Arguments:
- adjoint_now: float32 [4, 128, 64, 512], P('shot', 'space'), may hold values from -6 to 6
- adjoint_later: float32 [4, 128, 64, 512], P('shot', 'space'), may hold values from -6 to 6
- courant: float32 [128, 64, 512], P('space'), may hold values from 0.05 to 0.2
- checkpoint_codes: int32 [4, 6, 128, 64, 128], P('shot', None, 'space'), may hold values from -2147483648 to 2147483646
- scale_index: int32 [4, 6, 128, 256], P('shot', None, 'space'), may hold values from 0 to 63
- scale_table: float32 [64], replicated, may hold values from 0.001 to 0.01
- receiver_cell: int32 [4, 2048], P('shot', 'space'), may hold values from 0 to 4194303, as said below
- observed: float32 [4, 4, 2048], P('shot', None, 'space'), may hold values from -12 to 12
- source_cell: int32 [4, 3], P('shot'), may hold values from 0 to 511, as said below
Outputs:
- gradient: float32 [128, 64, 512], P('space', 'shot')
- adjoint_first: float32 [4, 128, 64, 512], P('shot', 'space')
- adjoint_second: float32 [4, 128, 64, 512], P('shot', 'space')
- misfit: float32 [], replicated
The draws below stay inside these ranges and needn't reach their ends.
Inputs may be any that keep to these rules, and one draw needn't show every extreme that they name: `receiver_cell`: for every r, entries r * 256 to (r + 1) * 256 - 1 of each shot's row are flat indices (z * 64 + y) * 512 + x of cells with r * 16 <= z < (r + 1) * 16. `source_cell`: column 0 is a z index below 128, column 1 a y index below 64, column 2 an x index below 512.
All inputs are finite; a program needn't handle non-finite values.
Results may differ from the reference program's by a relative error of at most 0.0001.
Values sent between devices are 32-bit elements; how exact they have to be, the bound alone decides.
No kernel may reach another device: no remote copies, remote signals or barrier semaphores. Data moves between devices by JAX's collectives and lax.ppermute only.
A program may use at most 128 MiB of HBM per device.

```python
import math
import jax
import jax.numpy as jnp

NX = 512
NY = 64
CZ = 16
ITERS = 4
QBLOCK = 128
SCALES = 64
MUTE = 8
REC_DEV = 256
LEVELS = 6
NZ = 128
SHOTS = 4
RECEIVERS = 2048


def draw_receiver_cell(key, part):
    keys = jax.random.split(jax.random.fold_in(key, 11), 3)
    slab = jnp.arange(RECEIVERS, dtype=jnp.int32) // REC_DEV
    depth = slab * CZ + jax.random.randint(keys[0], (SHOTS, RECEIVERS), 0, CZ)
    row = jax.random.randint(keys[1], (SHOTS, RECEIVERS), 0, NY)
    col = jax.random.randint(keys[2], (SHOTS, RECEIVERS), 0, NX)
    return ((depth * NY + row) * NX + col).astype(jnp.int32)


def draw_observed(key, part):
    ramp = 1.0 + 2.0 * jnp.arange(RECEIVERS, dtype=jnp.float32) / RECEIVERS
    base = jnp.clip(jax.random.normal(jax.random.fold_in(key, 22), (SHOTS, ITERS, RECEIVERS), jnp.float32), -4.0, 4.0)
    return (base * ramp).astype(jnp.float32)


def draw_source_cell(key, part):
    keys = jax.random.split(jax.random.fold_in(key, 31), 4)
    depth = jax.random.randint(keys[0], (SHOTS, 1), 0, NZ)
    row = jax.random.randint(keys[1], (SHOTS, 1), 0, NY)
    col = jax.random.randint(keys[2], (SHOTS, 1), 0, NX)
    chosen = jax.random.randint(keys[3], (), 0, SHOTS)
    marked = (jnp.arange(SHOTS, dtype=jnp.int32) == chosen).reshape(SHOTS, 1)
    depth = jnp.where(marked, NZ - 1, depth)
    row = jnp.where(marked, 0, row)
    return jnp.concatenate([depth, row, col], axis=1).astype(jnp.int32)


def set_ends(entries, key, smallest, largest):
    index_at = [jax.random.randint(jax.random.fold_in(key, axis), (), 0, length) for axis, length in enumerate(entries.shape)]
    longest = entries.shape.index(max(entries.shape))
    neighbour = index_at[:longest] + [(index_at[longest] + 1) % entries.shape[longest]] + index_at[longest + 1:]
    return entries.at[tuple(index_at)].set(smallest).at[tuple(neighbour)].set(largest)


def block_scale(rng, dims, cuts, low, high):
    loudness = 1.0
    for dim, parts in cuts:
        draws = jax.random.uniform(jax.random.fold_in(jax.random.fold_in(rng, 6), dim), (parts,), jnp.float32, low / len(cuts), high / len(cuts))
        loudness = loudness * jnp.repeat(jnp.exp(draws), dims[dim] // parts).reshape((-1,) + (1,) * (len(dims) - 1 - dim))
    return loudness


def scatter_about(key, shape, width, limit, shards=(), kind=jnp.bfloat16):
    gain = block_scale(key, shape, shards, -0.22, 0.18) if shards else 1.0
    values = jax.random.normal(key, shape, jnp.float32) * width * gain
    return jnp.minimum(jnp.maximum(values, -limit), limit).astype(kind)


def setup_inputs(seed: int = 0) -> dict:
    seeds = jax.random.split(jax.random.key(seed), 10)
    return {
        "adjoint_now": scatter_about(seeds[0], (SHOTS, NZ, NY, NX), 1.0, 6.0, ((0, 4), (1, 8)), jnp.float32),
        "adjoint_later": scatter_about(seeds[1], (SHOTS, NZ, NY, NX), 1.0, 6.0, ((0, 4), (1, 8)), jnp.float32),
        "courant": jnp.clip(jnp.exp(math.log(0.2) - 1.3862944 * jax.random.uniform(seeds[2], (NZ, NY, NX), jnp.float32) ** block_scale(seeds[2], (NZ, NY, NX), ((0, 8),), -0.2, 0.2)), 0.05, 0.2),
        "checkpoint_codes": set_ends(jax.random.randint(seeds[3], (SHOTS, LEVELS, NZ, NY, NX // 4), -2147483648, 2147483647), jax.random.fold_in(seeds[3], 1), -2147483648, 2147483646).astype(jnp.int32),
        "scale_index": set_ends(jax.random.randint(seeds[4], (SHOTS, LEVELS, NZ, NY * NX // QBLOCK), 0, SCALES), jax.random.fold_in(seeds[4], 1), 0, SCALES - 1).astype(jnp.int32),
        "scale_table": jnp.clip(jnp.exp(jax.random.uniform(seeds[5], (SCALES,), jnp.float32, math.log(0.001), math.log(0.01))), 0.001, 0.01),
        "receiver_cell": draw_receiver_cell(jax.random.fold_in(seeds[9], 71), 0),
        "observed": draw_observed(jax.random.fold_in(seeds[9], 71), 0),
        "source_cell": draw_source_cell(jax.random.fold_in(seeds[9], 71), 0),
    }


COEFFS = (-205.0 / 72.0, 8.0 / 5.0, -1.0 / 5.0, 8.0 / 315.0, -1.0 / 560.0)


def decode(words, index, table):
    planes = [jnp.bitwise_and(jnp.right_shift(words, 8 * m), 255) for m in range(4)]
    codes = jnp.concatenate(planes, axis=-1)
    centred = (codes - 128).astype(jnp.float32)
    depth, rows, cols = centred.shape
    scale = table[index]
    blocks = centred.reshape(depth, rows, cols // QBLOCK, QBLOCK) * scale.reshape(depth, rows, cols // QBLOCK, 1)
    return blocks.reshape(depth, rows, cols)


def laplace(field):
    padded = jnp.pad(field, 4)
    depth, rows, cols = field.shape
    total = 3.0 * COEFFS[0] * field
    for step in range(1, 5):
        total = total + COEFFS[step] * (padded[4 + step:4 + step + depth, 4:4 + rows, 4:4 + cols] + padded[4 - step:4 - step + depth, 4:4 + rows, 4:4 + cols])
        total = total + COEFFS[step] * (padded[4:4 + depth, 4 + step:4 + step + rows, 4:4 + cols] + padded[4:4 + depth, 4 - step:4 - step + rows, 4:4 + cols])
        total = total + COEFFS[step] * (padded[4:4 + depth, 4:4 + rows, 4 + step:4 + step + cols] + padded[4:4 + depth, 4:4 + rows, 4 - step:4 - step + cols])
    return total


def reference(adjoint_now, adjoint_later, courant, checkpoint_codes, scale_index, scale_table, receiver_cell, observed, source_cell):
    gradient = jnp.zeros((NZ, NY, NX), jnp.float32)
    misfit_sum = jnp.zeros((), jnp.float32)
    firsts = []
    seconds = []
    zpos = jnp.arange(NZ, dtype=jnp.int32).reshape(NZ, 1, 1)
    ypos = jnp.arange(NY, dtype=jnp.int32).reshape(1, NY, 1)
    xpos = jnp.arange(NX, dtype=jnp.int32).reshape(1, 1, NX)
    for shot in range(SHOTS):
        fields = [decode(checkpoint_codes[shot, level], scale_index[shot, level], scale_table) for level in range(ITERS + 2)]
        now = adjoint_now[shot]
        later = adjoint_later[shot]
        image = jnp.zeros((NZ, NY, NX), jnp.float32)
        cells = receiver_cell[shot]
        for step in range(ITERS):
            level = ITERS - step
            synthetic = jnp.take(fields[level].reshape(-1), cells)
            residual = synthetic - observed[shot, level - 1]
            misfit_sum = misfit_sum + jnp.sum(residual * residual)
            image = image + now * (fields[level + 1] - 2.0 * fields[level] + fields[level - 1])
            stepped = 2.0 * now - later + courant * laplace(now)
            stepped = stepped.reshape(-1).at[cells].add(residual).reshape(NZ, NY, NX)
            later = now
            now = stepped
        source = source_cell[shot]
        dist = ((zpos - source[0]) ** 2 + (ypos - source[1]) ** 2 + (xpos - source[2]) ** 2).astype(jnp.float32)
        mute = 1.0 - jnp.exp(-dist / (2.0 * MUTE * MUTE))
        gradient = gradient + image * mute
        firsts.append(now)
        seconds.append(later)
    misfit = 0.5 * misfit_sum / (SHOTS * ITERS * RECEIVERS)
    return gradient, jnp.stack(firsts), jnp.stack(seconds), misfit
```

```python
import functools

import jax
import jax.numpy as jnp
from jax import lax
from jax.experimental import pallas as pl
from jax.experimental.pallas import tpu as pltpu
from jax.sharding import PartitionSpec as P

ITERS = 4
MUTE = 8
LANES = 128
SUB = 8
REACH = 4

COEFFS = (-205.0 / 72.0, 8.0 / 5.0, -1.0 / 5.0, 8.0 / 315.0, -1.0 / 560.0)

VMEM = pl.BlockSpec(memory_space=pltpu.VMEM)
SMEM = pl.BlockSpec(memory_space=pltpu.SMEM)
ANY = pl.BlockSpec(memory_space=pl.ANY)


def params(mib):
    return pltpu.CompilerParams(vmem_limit_bytes=mib * 1024 * 1024)


def cost(us):
    return pl.CostEstimate(flops=int(us * 5e6), bytes_accessed=0, transcendentals=0)


def quotient(value, by):
    if by & (by - 1) == 0:
        return jnp.right_shift(value, by.bit_length() - 1)
    return value // by


def stack_planes(source, first, count, ypad):
    _, rows, cols = source.shape
    zero = jnp.zeros((SUB, LANES), jnp.float32)

    def step(j, carry):
        for t in range(cols // LANES):
            ypad[j, t, 0:SUB, :] = zero
            ypad[j, t, SUB + rows : 2 * SUB + rows, :] = zero
            ypad[j, t, SUB : SUB + rows, :] = source[first + j, :, t * LANES : (t + 1) * LANES]
        return carry

    lax.fori_loop(0, count, step, 0)


def update_planes(count, ypad, column, column_first, place, later, courant, added, new):
    _, rows, cols = new.shape
    tiles = cols // LANES
    lane = lax.broadcasted_iota(jnp.int32, (SUB, LANES), 1)
    zero = jnp.zeros((SUB, LANES), jnp.float32)

    def plane(j, carry):
        z = place + j
        for r in range(rows // SUB):
            y = slice(r * SUB, (r + 1) * SUB)
            centre = [ypad[j, t, SUB + r * SUB : 2 * SUB + r * SUB, :] for t in range(tiles)]
            total = [3.0 * COEFFS[0] * c for c in centre]
            for i in range(1, REACH + 1):
                right = [pltpu.roll(c, i, 1) for c in centre]
                left = [pltpu.roll(c, LANES - i, 1) for c in centre]
                for t in range(tiles):
                    x = slice(t * LANES, (t + 1) * LANES)
                    before = jnp.where(lane < i, right[t - 1] if t else zero, right[t])
                    after = jnp.where(
                        lane >= LANES - i, left[t + 1] if t + 1 < tiles else zero, left[t]
                    )
                    near = ypad[j, t, SUB + r * SUB - i : 2 * SUB + r * SUB - i, :]
                    far = ypad[j, t, SUB + r * SUB + i : 2 * SUB + r * SUB + i, :]
                    below = column[column_first + j - i, y, x]
                    above = column[column_first + j + i, y, x]
                    total[t] = total[t] + COEFFS[i] * (
                        ((before + after) + (near + far)) + (below + above)
                    )
            for t in range(tiles):
                x = slice(t * LANES, (t + 1) * LANES)
                value = (2.0 * centre[t] - later[z, y, x]) + (
                    courant[z, y, x] * total[t] + added[z, y, x]
                )
                new[j, y, x] = value
        return carry

    lax.fori_loop(0, count, plane, 0)


def inner_kernel(now, later, courant, added, new, ypad):
    depth = now.shape[0]
    count = depth - 2 * REACH
    stack_planes(now, REACH, count, ypad)
    update_planes(count, ypad, now, REACH, REACH, later, courant, added, new)


def edge(place, now, halo, later, courant, added, strip, ypad, column):
    depth, rows, cols = now.shape
    first = place[0]
    high = first > 0
    halo_at = jnp.where(high, 2 * REACH, 0)
    own_at = jnp.where(high, 0, REACH)
    own_first = jnp.where(high, depth - 2 * REACH, 0)

    def copy_halo(j, carry):
        column[halo_at + j] = halo[j]
        return carry

    def copy_own(j, carry):
        column[own_at + j] = now[own_first + j]
        return carry

    lax.fori_loop(0, REACH, copy_halo, 0)
    lax.fori_loop(0, 2 * REACH, copy_own, 0)
    stack_planes(now, first, REACH, ypad)
    update_planes(REACH, ypad, column, REACH, first, later, courant, added, strip)


def pair_kernel(place, now, halo, later, courant, added, strip, ypad, column):
    edge(place, now, halo, later, courant, added, strip, ypad, column)


def cross_kernel(
    place, now, halo, later, courant, added, middle, other, new, strip, ypad, column
):
    depth = now.shape[0]
    edge(place, now, halo, later, courant, added, strip, ypad, column)
    first = place[0]
    opposite = depth - REACH - first

    def copy_edges(j, carry):
        new[first + j] = strip[j]
        new[opposite + j] = other[j]
        return carry

    def copy_middle(j, carry):
        new[REACH + j] = middle[j]
        return carry

    lax.fori_loop(0, REACH, copy_edges, 0)
    lax.fori_loop(0, depth - 2 * REACH, copy_middle, 0)


def source_kernel(
    first, cell, codes, index, table, observed, *refs
):
    spread = refs[:ITERS]
    squares = refs[ITERS]
    packed, onehot = refs[ITERS + 1 :]
    _, depth, rows, words = codes.shape
    cols = spread[0].shape[2]
    tiles = cols // LANES
    count = cell.shape[1]
    flat = cell[...] - first[0]
    zy = quotient(flat, cols)
    x = flat - zy * cols
    z = quotient(zy, rows)
    block = (zy - z * rows) * tiles + quotient(x, LANES)
    packed[...] = jnp.zeros(packed.shape, jnp.float32)
    for k, line in enumerate((x, zy, z, block)):
        packed[k : k + 1, :] = line.astype(jnp.float32)
    packed[SUB : SUB + ITERS, :] = observed[...]
    turned = jnp.concatenate(
        [packed[:, k * LANES : (k + 1) * LANES].T for k in range(count // LANES)], axis=0
    )
    x_col, zy_col, z_col, block_col = (turned[:, k : k + 1].astype(jnp.int32) for k in range(4))
    one = jnp.ones((), jnp.float32)
    none = jnp.zeros((), jnp.float32)

    def hot(shape, col):
        return jnp.where(lax.broadcasted_iota(jnp.int32, shape, 1) == col, one, none)

    onehot[...] = hot((count, depth * rows), zy_col).astype(jnp.bfloat16)
    at_z = hot((count, depth), z_col).astype(jnp.bfloat16)
    at_x = lax.broadcasted_iota(jnp.int32, (count, cols), 1) == x_col
    at_block = lax.broadcasted_iota(jnp.int32, (count, rows * tiles), 1) == block_col
    total = jnp.zeros((count, 1), jnp.float32)
    parts = []
    for step in range(ITERS):
        level = ITERS - step
        word = codes[level].reshape(depth * rows, words)
        code = jnp.concatenate(
            [
                (jnp.bitwise_and(jnp.right_shift(word, 8 * m), 255) - 128)
                .astype(jnp.float32)
                .astype(jnp.bfloat16)
                for m in range(tiles)
            ],
            axis=1,
        )
        lines = jnp.dot(onehot[...], code, preferred_element_type=jnp.float32)
        picked = jnp.sum(jnp.where(at_x, lines, 0.0), axis=1, keepdims=True)
        entries = jnp.dot(
            at_z,
            index[level].astype(jnp.float32).astype(jnp.bfloat16),
            preferred_element_type=jnp.float32,
        )
        entry = jnp.sum(jnp.where(at_block, entries, 0.0), axis=1, keepdims=True)
        at_entry = lax.broadcasted_iota(jnp.int32, (count, LANES), 1) == entry.astype(jnp.int32)
        scale = jnp.sum(jnp.where(at_entry, table[...], 0.0), axis=1, keepdims=True)
        residual = picked * scale - turned[:, SUB + level - 1 : SUB + level]
        total = total + residual * residual
        dense = jnp.where(at_x, residual, 0.0)
        head = dense.astype(jnp.bfloat16)
        rest = dense - head.astype(jnp.float32)
        middle = rest.astype(jnp.bfloat16)
        tail = (rest - middle.astype(jnp.float32)).astype(jnp.bfloat16)
        parts.append((head, middle, tail))
    squares[...] = jnp.broadcast_to(jnp.sum(total, axis=0, keepdims=True), squares.shape)

    group = 4

    for step in range(ITERS):
        pieces = parts[step]

        def planes(k, carry, out=spread[step], pieces=pieces):
            rank = lax.broadcasted_iota(jnp.int32, (group * rows, count), 0) + k * (group * rows)
            at = jnp.where(rank == zy, one, none).astype(jnp.bfloat16)
            value = sum(
                jnp.dot(at, piece, preferred_element_type=jnp.float32) for piece in pieces
            )
            out[pl.ds(k * group, group)] = value.reshape(group, rows, cols)
            return carry

        lax.fori_loop(0, depth // group, planes, 0)


def image_kernel(
    place, codes, index, table, w0, w1, w2, image, last, packed, turned, ey
):
    levels, depth, rows, words = codes.shape
    cols = image.shape[2]
    tiles = cols // LANES
    first_z, source_z, source_y, source_x = (place[k] for k in range(4))
    scale_by = -1.0 / (2.0 * MUTE * MUTE)
    lane = lax.broadcasted_iota(jnp.int32, (SUB, LANES), 1)

    def bell(distance):
        off = distance.astype(jnp.float32)
        return jnp.exp(off * off * scale_by)

    packed[...] = jnp.zeros(packed.shape, jnp.float32)
    lines = levels * depth
    chosen = index[...].reshape(lines, rows * tiles)
    across = jnp.broadcast_to(table[...], (lines, LANES))
    for h in range(rows * tiles // LANES):
        cut = slice(h * LANES, (h + 1) * LANES)
        packed[0:lines, cut] = jnp.take_along_axis(
            across, chosen[:, cut], axis=1, mode="promise_in_bounds"
        )
        turned[cut, :] = packed[:, cut].T
    ey[...] = bell(lax.broadcasted_iota(jnp.int32, (rows, LANES), 0) - source_y)
    ex = [bell(lane + (t * LANES) - source_x) for t in range(tiles)]

    def plane(z, carry):
        ez = bell(jnp.full((SUB, LANES), first_z + z - source_z, jnp.int32))
        for r in range(rows // SUB):
            y = slice(r * SUB, (r + 1) * SUB)
            word = [codes[level, z, y, :] for level in range(levels)]
            down = ez * ey[y, :]
            for t in range(tiles):
                x = slice(t * LANES, (t + 1) * LANES)
                scales = pltpu.roll(
                    turned[pl.ds(t + tiles * SUB * r, SUB, stride=tiles), :],
                    lax.rem(LANES - z, LANES),
                    1,
                )
                field = []
                for level in range(levels):
                    code = jnp.bitwise_and(jnp.right_shift(word[level], 8 * t), 255) - 128
                    scale = jnp.broadcast_to(
                        scales[:, level * depth : level * depth + 1], (SUB, LANES)
                    )
                    field.append(code.astype(jnp.float32) * scale)
                bend = [
                    None if k in (0, levels - 1)
                    else (field[k + 1] - 2.0 * field[k]) + field[k - 1]
                    for k in range(levels)
                ]
                mute = 1.0 - down * ex[t]
                value = w0[z, y, x] * bend[ITERS]
                value = value + w1[z, y, x] * bend[ITERS - 1]
                value = value + w2[z, y, x] * bend[ITERS - 2]
                image[z, y, x] = mute * value
                last[z, y, x] = mute * bend[ITERS - 3]
        return carry

    lax.fori_loop(0, depth, plane, 0)


def split_kernel(side, image, last, w3, kept, sent):
    half, depth, block, cols = kept.shape
    mine = side[0]

    def plane(z, carry):
        for q in range(half):
            for out, which in ((kept, mine), (sent, 1 - mine)):
                y = pl.ds(pl.multiple_of((2 * q + which) * block, SUB), block)
                out[q, z] = image[z, y, :] + last[z, y, :] * w3[z, y, :]
        return carry

    lax.fori_loop(0, depth, plane, 0)


def summed(value, axis):
    count = lax.axis_size(axis)
    if count & (count - 1):
        return lax.psum(value, axis)
    hop = 1
    while hop < count:
        value = value + lax.ppermute(value, axis, [(i, i ^ hop) for i in range(count)])
        hop *= 2
    return value


def body(
    adjoint_now,
    adjoint_later,
    courant,
    checkpoint_codes,
    scale_index,
    scale_table,
    receiver_cell,
    observed,
    source_cell,
):
    now = adjoint_now[0]
    later = adjoint_later[0]
    codes = checkpoint_codes[0]
    index = scale_index[0]
    depth, rows, cols = now.shape
    levels = codes.shape[0]
    tiles = cols // LANES
    receivers = receiver_cell.shape[1]
    slabs = lax.axis_size("space")
    shots = lax.axis_size("shot")
    slab = lax.axis_index("space")
    shot = lax.axis_index("shot")
    even = slab % 2 == 0
    pair_place = jnp.where(even, depth - REACH, 0).astype(jnp.int32)
    cross_place = (depth - REACH) - pair_place
    pairs = [(i, i ^ 1) for i in range(slabs) if i ^ 1 < slabs]
    crosses = [(i, i + 1) for i in range(1, slabs - 1, 2)]
    crosses = crosses + [(b, a) for a, b in crosses]
    field = jax.ShapeDtypeStruct((depth, rows, cols), jnp.float32)
    strip = jax.ShapeDtypeStruct((REACH, rows, cols), jnp.float32)
    first_z = slab * depth

    def pair_exchange(block):
        return lax.ppermute(block, "space", pairs)

    def cross_exchange(block):
        return lax.ppermute(block, "space", crosses)

    ypad = (tiles, rows + 2 * SUB, LANES)
    middle = jax.ShapeDtypeStruct((depth - 2 * REACH, rows, cols), jnp.float32)
    edge_scratch = [
        pltpu.VMEM((REACH,) + ypad, jnp.float32),
        pltpu.VMEM((3 * REACH, rows, cols), jnp.float32),
    ]
    inner = pl.pallas_call(
        inner_kernel,
        out_shape=middle,
        in_specs=[VMEM] * 4,
        out_specs=VMEM,
        scratch_shapes=[pltpu.VMEM((depth - 2 * REACH,) + ypad, jnp.float32)],
        compiler_params=params(20),
        cost_estimate=cost(3),
        name="inner",
    )
    pair = pl.pallas_call(
        pair_kernel,
        out_shape=strip,
        in_specs=[SMEM] + [VMEM] * 5,
        out_specs=VMEM,
        scratch_shapes=edge_scratch,
        compiler_params=params(20),
        cost_estimate=cost(2),
        name="pair",
    )
    cross = pl.pallas_call(
        cross_kernel,
        out_shape=(field, strip),
        in_specs=[SMEM] + [VMEM] * 7,
        out_specs=(VMEM, VMEM),
        scratch_shapes=edge_scratch,
        compiler_params=params(20),
        cost_estimate=cost(2),
        name="cross",
    )

    pair_halo = pair_exchange(lax.dynamic_slice_in_dim(now, pair_place, REACH, 0))
    cross_halo = cross_exchange(lax.dynamic_slice_in_dim(now, cross_place, REACH, 0))

    table = jnp.pad(scale_table, (0, LANES - scale_table.shape[0])).reshape(1, LANES)
    *added, squares = pl.pallas_call(
        source_kernel,
        out_shape=[field] * ITERS + [jax.ShapeDtypeStruct((SUB, LANES), jnp.float32)],
        in_specs=[SMEM] + [VMEM] * 5,
        out_specs=[VMEM] * (ITERS + 1),
        scratch_shapes=[
            pltpu.VMEM((LANES, receivers), jnp.float32),
            pltpu.VMEM((receivers, depth * rows), jnp.bfloat16),
        ],
        compiler_params=params(28),
        cost_estimate=cost(8),
        name="sources",
    )(
        (first_z * (rows * cols)).reshape(1).astype(jnp.int32),
        receiver_cell,
        codes,
        index,
        table,
        observed[0],
    )

    waves = [now]
    for step in range(ITERS):
        now = waves[-1]
        within = inner(now, later, courant, added[step])
        pair_sent = pair(pair_place.reshape(1), now, pair_halo, later, courant, added[step])
        if step + 1 < ITERS:
            pair_halo = pair_exchange(pair_sent)
        new, cross_sent = cross(
            cross_place.reshape(1),
            now,
            cross_halo,
            later,
            courant,
            added[step],
            within,
            pair_sent,
        )
        if step + 1 < ITERS:
            cross_halo = cross_exchange(cross_sent)
        later = now
        waves.append(new)

    place = jnp.concatenate([first_z.reshape(1).astype(jnp.int32), source_cell[0]])
    image, last = pl.pallas_call(
        image_kernel,
        out_shape=(field, field),
        in_specs=[SMEM] + [VMEM] * 6,
        out_specs=(VMEM, VMEM),
        scratch_shapes=[
            pltpu.VMEM((LANES, rows * tiles), jnp.float32),
            pltpu.VMEM((rows * tiles, LANES), jnp.float32),
            pltpu.VMEM((rows, LANES), jnp.float32),
        ],
        compiler_params=params(28),
        cost_estimate=cost(5),
        name="image",
    )(place, codes, index, table, waves[0], waves[1], waves[2])

    block = rows // shots
    part = jax.ShapeDtypeStruct((shots // 2, depth, block, cols), jnp.float32)
    kept, sent = pl.pallas_call(
        split_kernel,
        out_shape=(part, part),
        in_specs=[SMEM] + [VMEM] * 3,
        out_specs=(VMEM, VMEM),
        compiler_params=params(20),
        cost_estimate=cost(2),
        name="split",
    )((shot % 2).reshape(1).astype(jnp.int32), image, last, waves[3])
    hop = 1
    while True:
        kept = kept + lax.ppermute(sent, "shot", [(i, i ^ hop) for i in range(shots)])
        hop *= 2
        if hop >= shots:
            break
        mine = (shot // hop) % 2
        halves = kept.reshape((kept.shape[0] // 2, 2) + kept.shape[1:])
        kept = lax.dynamic_index_in_dim(halves, mine, 1, keepdims=False)
        sent = lax.dynamic_index_in_dim(halves, 1 - mine, 1, keepdims=False)
    gradient = kept[0]

    squares = summed(summed(squares, "space"), "shot")
    misfit = 0.5 * squares[0, 0] / (shots * ITERS * receivers * slabs)
    return (gradient, waves[4][None], waves[3][None], misfit)


def solution(mesh):
    placed = (
        P("shot", "space", None, None),
        P("shot", "space", None, None),
        P("space", None, None),
        P("shot", None, "space", None, None),
        P("shot", None, "space", None),
        P(),
        P("shot", "space"),
        P("shot", None, "space"),
        P("shot", None),
    )
    return jax.shard_map(
        body,
        mesh=mesh,
        in_specs=placed,
        out_specs=(
            P("space", "shot", None),
            P("shot", "space", None, None),
            P("shot", "space", None, None),
            P(),
        ),
        check_vma=False,
    )
```

```python
import functools

import jax
import jax.numpy as jnp
from jax import lax
from jax.experimental import pallas as pl
from jax.experimental.pallas import tpu as pltpu
from jax.sharding import PartitionSpec as P


ITERS = 4
MUTE = 8
LANES = 128
SUB = 8
REACH = 4

COEFFS = (-205.0 / 72.0, 8.0 / 5.0, -1.0 / 5.0, 8.0 / 315.0, -1.0 / 560.0)

VMEM = pl.BlockSpec(memory_space=pltpu.VMEM)
SMEM = pl.BlockSpec(memory_space=pltpu.SMEM)
ANY = pl.BlockSpec(memory_space=pl.ANY)


def params(mib):
    return pltpu.CompilerParams(vmem_limit_bytes=mib * 1024 * 1024)


def cost(us):
    return pl.CostEstimate(flops=int(us * 5e6), bytes_accessed=0, transcendentals=0)


def quotient(value, by):
    if by & (by - 1) == 0:
        return jnp.right_shift(value, by.bit_length() - 1)
    return value // by


def stack_planes(source, first, count, ypad):
    _, rows, cols = source.shape
    zero = jnp.zeros((SUB, LANES), jnp.float32)

    def step(j, carry):
        for t in range(cols // LANES):
            ypad[j, t, 0:SUB, :] = zero
            ypad[j, t, SUB + rows : 2 * SUB + rows, :] = zero
            ypad[j, t, SUB : SUB + rows, :] = source[first + j, :, t * LANES : (t + 1) * LANES]
        return carry

    lax.fori_loop(0, count, step, 0)


def update_planes(count, ypad, column, column_first, place, later, courant, added, new):
    _, rows, cols = new.shape
    tiles = cols // LANES
    lane = lax.broadcasted_iota(jnp.int32, (SUB, LANES), 1)
    zero = jnp.zeros((SUB, LANES), jnp.float32)

    def plane(j, carry):
        z = place + j
        for r in range(rows // SUB):
            y = slice(r * SUB, (r + 1) * SUB)
            centre = [ypad[j, t, SUB + r * SUB : 2 * SUB + r * SUB, :] for t in range(tiles)]
            total = [3.0 * COEFFS[0] * c for c in centre]
            for i in range(1, REACH + 1):
                right = [pltpu.roll(c, i, 1) for c in centre]
                left = [pltpu.roll(c, LANES - i, 1) for c in centre]
                for t in range(tiles):
                    x = slice(t * LANES, (t + 1) * LANES)
                    before = jnp.where(lane < i, right[t - 1] if t else zero, right[t])
                    after = jnp.where(
                        lane >= LANES - i, left[t + 1] if t + 1 < tiles else zero, left[t]
                    )
                    near = ypad[j, t, SUB + r * SUB - i : 2 * SUB + r * SUB - i, :]
                    far = ypad[j, t, SUB + r * SUB + i : 2 * SUB + r * SUB + i, :]
                    below = column[column_first + j - i, y, x]
                    above = column[column_first + j + i, y, x]
                    total[t] = total[t] + COEFFS[i] * (
                        ((before + after) + (near + far)) + (below + above)
                    )
            for t in range(tiles):
                x = slice(t * LANES, (t + 1) * LANES)
                value = (2.0 * centre[t] - later[z, y, x]) + (
                    courant[z, y, x] * total[t] + added[z, y, x]
                )
                new[j, y, x] = value
        return carry

    lax.fori_loop(0, count, plane, 0)


def inner_kernel(now, later, courant, added, new, ypad):
    depth = now.shape[0]
    count = depth - 2 * REACH
    stack_planes(now, REACH, count, ypad)
    update_planes(count, ypad, now, REACH, REACH, later, courant, added, new)


def edge(place, now, halo, later, courant, added, strip, ypad, column):
    depth, _, _ = now.shape
    first = place[0]
    high = first > 0
    halo_at = jnp.where(high, 2 * REACH, 0)
    own_at = jnp.where(high, 0, REACH)
    own_first = jnp.where(high, depth - 2 * REACH, 0)

    def copy_halo(j, carry):
        column[halo_at + j] = halo[j]
        return carry

    def copy_own(j, carry):
        column[own_at + j] = now[own_first + j]
        return carry

    lax.fori_loop(0, REACH, copy_halo, 0)
    lax.fori_loop(0, 2 * REACH, copy_own, 0)
    stack_planes(now, first, REACH, ypad)
    update_planes(REACH, ypad, column, REACH, first, later, courant, added, strip)


def pair_kernel(place, now, halo, later, courant, added, strip, ypad, column):
    edge(place, now, halo, later, courant, added, strip, ypad, column)


def cross_kernel(
    place, now, halo, later, courant, added, middle, other, new, strip, ypad, column
):
    depth = now.shape[0]
    edge(place, now, halo, later, courant, added, strip, ypad, column)
    first = place[0]
    opposite = depth - REACH - first

    def copy_edges(j, carry):
        new[first + j] = strip[j]
        new[opposite + j] = other[j]
        return carry

    def copy_middle(j, carry):
        new[REACH + j] = middle[j]
        return carry

    lax.fori_loop(0, REACH, copy_edges, 0)
    lax.fori_loop(0, depth - 2 * REACH, copy_middle, 0)


def source_kernel(
    first, cell, codes, index, table, observed, *refs
):
    spread = refs[:ITERS]
    squares = refs[ITERS]
    packed, onehot = refs[ITERS + 1 :]
    _, depth, rows, words = codes.shape
    cols = spread[0].shape[2]
    tiles = cols // LANES
    count = cell.shape[1]
    flat = cell[...] - first[0]
    zy = quotient(flat, cols)
    x = flat - zy * cols
    z = quotient(zy, rows)
    block = (zy - z * rows) * tiles + quotient(x, LANES)
    packed[...] = jnp.zeros(packed.shape, jnp.float32)
    for k, line in enumerate((x, zy, z, block)):
        packed[k : k + 1, :] = line.astype(jnp.float32)
    packed[SUB : SUB + ITERS, :] = observed[...]
    turned = jnp.concatenate(
        [packed[:, k * LANES : (k + 1) * LANES].T for k in range(count // LANES)], axis=0
    )
    x_col, zy_col, z_col, block_col = (turned[:, k : k + 1].astype(jnp.int32) for k in range(4))
    one = jnp.ones((), jnp.float32)
    none = jnp.zeros((), jnp.float32)

    def hot(shape, col):
        return jnp.where(lax.broadcasted_iota(jnp.int32, shape, 1) == col, one, none)

    onehot[...] = hot((count, depth * rows), zy_col).astype(jnp.bfloat16)
    at_z = hot((count, depth), z_col).astype(jnp.bfloat16)
    at_x = lax.broadcasted_iota(jnp.int32, (count, cols), 1) == x_col
    at_block = lax.broadcasted_iota(jnp.int32, (count, rows * tiles), 1) == block_col
    total = jnp.zeros((count, 1), jnp.float32)
    parts = []
    for step in range(ITERS):
        level = ITERS - step
        word = codes[level].reshape(depth * rows, words)
        code = jnp.concatenate(
            [
                (jnp.bitwise_and(jnp.right_shift(word, 8 * m), 255) - 128)
                .astype(jnp.float32)
                .astype(jnp.bfloat16)
                for m in range(tiles)
            ],
            axis=1,
        )
        lines = jnp.dot(onehot[...], code, preferred_element_type=jnp.float32)
        picked = jnp.sum(jnp.where(at_x, lines, 0.0), axis=1, keepdims=True)
        entries = jnp.dot(
            at_z,
            index[level].astype(jnp.float32).astype(jnp.bfloat16),
            preferred_element_type=jnp.float32,
        )
        entry = jnp.sum(jnp.where(at_block, entries, 0.0), axis=1, keepdims=True)
        at_entry = lax.broadcasted_iota(jnp.int32, (count, table.shape[1]), 1) == entry.astype(
            jnp.int32
        )
        scale = jnp.sum(jnp.where(at_entry, table[...], 0.0), axis=1, keepdims=True)
        residual = picked * scale - turned[:, SUB + level - 1 : SUB + level]
        total = total + residual * residual
        dense = jnp.where(at_x, residual, 0.0)
        head = dense.astype(jnp.bfloat16)
        rest = dense - head.astype(jnp.float32)
        middle = rest.astype(jnp.bfloat16)
        tail = (rest - middle.astype(jnp.float32)).astype(jnp.bfloat16)
        parts.append((head, middle, tail))
    squares[...] = jnp.broadcast_to(jnp.sum(total, axis=0, keepdims=True), squares.shape)

    group = 4

    for step in range(ITERS):
        pieces = parts[step]

        def planes(k, carry, out=spread[step], pieces=pieces):
            rank = lax.broadcasted_iota(jnp.int32, (group * rows, count), 0) + k * (group * rows)
            at = jnp.where(rank == zy, one, none).astype(jnp.bfloat16)
            value = sum(
                jnp.dot(at, piece, preferred_element_type=jnp.float32) for piece in pieces
            )
            out[pl.ds(k * group, group)] = value.reshape(group, rows, cols)
            return carry

        lax.fori_loop(0, depth // group, planes, 0)


def image_kernel(
    first, source, codes, index, table, w0, w1, w2, image, last, packed, turned, ey, held, field
):
    levels, depth, rows, _ = codes.shape
    cols = image.shape[2]
    tiles = cols // LANES
    first_z = first[0]
    source_z, source_y, source_x = (source[0, k] for k in range(3))
    scale_by = -1.0 / (2.0 * MUTE * MUTE)
    lane = lax.broadcasted_iota(jnp.int32, (SUB, LANES), 1)

    def bell(distance):
        off = distance.astype(jnp.float32)
        return jnp.exp(off * off * scale_by)

    packed[...] = jnp.zeros(packed.shape, jnp.float32)
    lines = levels * depth
    chosen = index[...].reshape(lines, rows * tiles)
    held[0:1, 0 : table.shape[1]] = table[...]
    across = jnp.broadcast_to(held[0:1, :], (lines, LANES))
    for h in range(rows * tiles // LANES):
        cut = slice(h * LANES, (h + 1) * LANES)
        packed[0:lines, cut] = jnp.take_along_axis(
            across, chosen[:, cut], axis=1, mode="promise_in_bounds"
        )
        turned[cut, :] = packed[:, cut].T
    ey[...] = bell(lax.broadcasted_iota(jnp.int32, (rows, LANES), 0) - source_y)
    ex = [bell(lane + (t * LANES) - source_x) for t in range(tiles)]

    def plane(z, carry):
        turn = lax.rem(LANES - z, LANES)
        for t in range(tiles):
            for r in range(rows // SUB):
                held[t * rows + r * SUB : t * rows + (r + 1) * SUB, :] = pltpu.roll(
                    turned[pl.ds(t + tiles * SUB * r, SUB, stride=tiles), :], turn, 1
                )
        for level in range(levels):
            lane_at = slice(level * depth, level * depth + 1)
            for r in range(rows // SUB):
                y = slice(r * SUB, (r + 1) * SUB)
                word = codes[level, z, y, :]
                for t in range(tiles):
                    at = slice(t * rows + r * SUB, t * rows + (r + 1) * SUB)
                    scale = jnp.broadcast_to(held[at, lane_at], (SUB, LANES))
                    code = jnp.bitwise_and(jnp.right_shift(word, 8 * t), 255) - 128
                    field[level, y, t * LANES : (t + 1) * LANES] = code.astype(jnp.float32) * scale
        ez = bell(jnp.full((SUB, LANES), first_z + z - source_z, jnp.int32))
        for r in range(rows // SUB):
            y = slice(r * SUB, (r + 1) * SUB)
            down = ez * ey[y, :]
            for t in range(tiles):
                x = slice(t * LANES, (t + 1) * LANES)
                value = [field[level, y, x] for level in range(levels)]
                bend = [
                    None if k in (0, levels - 1)
                    else (value[k + 1] - 2.0 * value[k]) + value[k - 1]
                    for k in range(levels)
                ]
                mute = 1.0 - down * ex[t]
                terms = w0[z, y, x] * bend[ITERS]
                terms = terms + w1[z, y, x] * bend[ITERS - 1]
                terms = terms + w2[z, y, x] * bend[ITERS - 2]
                image[z, y, x] = mute * terms
                last[z, y, x] = mute * bend[ITERS - 3]
        return carry

    lax.fori_loop(0, depth, plane, 0)


def cut_kernel(place, now, after, strip):
    del after
    first = place[0]

    def step(j, carry):
        strip[j] = now[first + j]
        return carry

    lax.fori_loop(0, REACH, step, 0)


def split_kernel(side, image, last, w3, kept, sent):
    half, depth, block, _ = kept.shape
    mine = side[0]

    def plane(z, carry):
        for q in range(half):
            for out, which in ((kept, mine), (sent, 1 - mine)):
                y = pl.ds(pl.multiple_of((2 * q + which) * block, SUB), block)
                out[q, z] = image[z, y, :] + last[z, y, :] * w3[z, y, :]
        return carry

    lax.fori_loop(0, depth, plane, 0)


def halve_kernel(side, kept, arrived, keep, send):
    half, depth, _, _ = keep.shape
    mine = side[0]

    def plane(z, carry):
        for q in range(half):
            for out, which in ((keep, mine), (send, 1 - mine)):
                out[q, z] = kept[2 * q + which, z] + arrived[2 * q + which, z]
        return carry

    lax.fori_loop(0, depth, plane, 0)


def add_kernel(one, other, out):
    def plane(z, carry):
        out[z] = one[z] + other[z]
        return carry

    lax.fori_loop(0, out.shape[0], plane, 0)


def tile_add_kernel(one, other, out):
    out[...] = one[...] + other[...]


def scalar_kernel(factor, one, other, out):
    out[0, 0] = ((one[...] + other[...]) * factor)[0, 0]


def misfit_of(squares, factor):
    hops = []
    for axis, name in (("space", "m"), ("shot", "n")):
        count = lax.axis_size(axis)
        if count & (count - 1):
            squares = lax.psum(squares, axis)
            continue
        hop = 1
        while hop < count:
            hops.append((axis, f"{name}{hop}", [(i, i ^ hop) for i in range(count)]))
            hop *= 2
    for k, (axis, name, moves) in enumerate(hops):
        arrived = lax.ppermute(squares, axis, moves)
        last = k + 1 == len(hops)
        squares = pl.pallas_call(
            functools.partial(scalar_kernel, factor) if last else tile_add_kernel,
            out_shape=jax.ShapeDtypeStruct((1, 1) if last else squares.shape, jnp.float32),
            in_specs=[VMEM] * 2,
            out_specs=SMEM if last else VMEM,
            compiler_params=params(4),
            cost_estimate=cost(0.2),
            name="tally",
        )(squares, arrived)
    return squares


def body(
    adjoint_now,
    adjoint_later,
    courant,
    checkpoint_codes,
    scale_index,
    scale_table,
    receiver_cell,
    observed,
    source_cell,
):
    now = adjoint_now[0]
    later = adjoint_later[0]
    codes = checkpoint_codes[0]
    index = scale_index[0]
    depth, rows, cols = now.shape
    levels = codes.shape[0]
    tiles = cols // LANES
    receivers = receiver_cell.shape[1]
    slabs = lax.axis_size("space")
    shots = lax.axis_size("shot")
    slab = lax.axis_index("space")
    shot = lax.axis_index("shot")
    even = slab % 2 == 0
    pair_place = jnp.where(even, depth - REACH, 0).astype(jnp.int32)
    cross_place = (depth - REACH) - pair_place
    pairs = [(i, i ^ 1) for i in range(slabs) if i ^ 1 < slabs]
    crosses = [(i, i + 1) for i in range(1, slabs - 1, 2)]
    crosses = crosses + [(b, a) for a, b in crosses]
    field = jax.ShapeDtypeStruct((depth, rows, cols), jnp.float32)
    strip = jax.ShapeDtypeStruct((REACH, rows, cols), jnp.float32)
    first_z = slab * depth

    def pair_exchange(block):
        return lax.ppermute(block, "space", pairs)

    def cross_exchange(block):
        return lax.ppermute(block, "space", crosses)

    ypad = (tiles, rows + 2 * SUB, LANES)
    middle = jax.ShapeDtypeStruct((depth - 2 * REACH, rows, cols), jnp.float32)
    edge_scratch = [
        pltpu.VMEM((REACH,) + ypad, jnp.float32),
        pltpu.VMEM((3 * REACH, rows, cols), jnp.float32),
    ]
    inner = pl.pallas_call(
        inner_kernel,
        out_shape=middle,
        in_specs=[VMEM] * 4,
        out_specs=VMEM,
        scratch_shapes=[pltpu.VMEM((depth - 2 * REACH,) + ypad, jnp.float32)],
        compiler_params=params(10),
        cost_estimate=cost(3),
        name="inner",
    )
    pair = pl.pallas_call(
        pair_kernel,
        out_shape=strip,
        in_specs=[SMEM] + [VMEM] * 5,
        out_specs=VMEM,
        scratch_shapes=edge_scratch,
        compiler_params=params(10),
        cost_estimate=cost(2),
        name="pair",
    )
    cross = pl.pallas_call(
        cross_kernel,
        out_shape=(field, strip),
        in_specs=[SMEM] + [VMEM] * 7,
        out_specs=(VMEM, VMEM),
        scratch_shapes=edge_scratch,
        compiler_params=params(10),
        cost_estimate=cost(2),
        name="cross",
    )

    pair_halo = pair_exchange(lax.dynamic_slice_in_dim(now, pair_place, REACH, 0))

    table = scale_table.reshape(1, scale_table.shape[0])
    sources = pl.pallas_call(
        source_kernel,
        out_shape=[field] * ITERS + [jax.ShapeDtypeStruct((SUB, LANES), jnp.float32)],
        in_specs=[SMEM] + [VMEM] * 5,
        out_specs=[VMEM] * (ITERS + 1),
        scratch_shapes=[
            pltpu.VMEM((LANES, receivers), jnp.float32),
            pltpu.VMEM((receivers, depth * rows), jnp.bfloat16),
        ],
        compiler_params=params(14),
        cost_estimate=cost(8),
        name="sources",
    )
    *added, squares = sources(
        (first_z * (rows * cols)).reshape(1).astype(jnp.int32),
        receiver_cell,
        codes,
        index,
        table,
        observed[0],
    )

    cross_sent = pl.pallas_call(
        cut_kernel,
        out_shape=strip,
        in_specs=[SMEM, VMEM, ANY],
        out_specs=VMEM,
        compiler_params=params(6),
        cost_estimate=cost(1),
        name="cut",
    )(cross_place.reshape(1), now, squares)
    cross_halo = cross_exchange(cross_sent)

    waves = [now]
    for step in range(ITERS):
        now = waves[-1]
        within = inner(now, later, courant, added[step])
        pair_sent = pair(pair_place.reshape(1), now, pair_halo, later, courant, added[step])
        if step + 1 < ITERS:
            pair_halo = pair_exchange(pair_sent)
        new, cross_sent = cross(
            cross_place.reshape(1),
            now,
            cross_halo,
            later,
            courant,
            added[step],
            within,
            pair_sent,
        )
        if step + 1 < ITERS:
            cross_halo = cross_exchange(cross_sent)
        later = now
        waves.append(new)

    images = pl.pallas_call(
        image_kernel,
        out_shape=(field, field),
        in_specs=[SMEM] * 2 + [VMEM] * 6,
        out_specs=(VMEM, VMEM),
        scratch_shapes=[
            pltpu.VMEM((LANES, rows * tiles), jnp.float32),
            pltpu.VMEM((rows * tiles, LANES), jnp.float32),
            pltpu.VMEM((rows, LANES), jnp.float32),
            pltpu.VMEM((tiles * rows, LANES), jnp.float32),
            pltpu.VMEM((levels, rows, cols), jnp.float32),
        ],
        compiler_params=params(12),
        cost_estimate=cost(5),
        name="image",
    )
    image, last = images(
        first_z.reshape(1).astype(jnp.int32),
        source_cell,
        codes,
        index,
        table,
        waves[0],
        waves[1],
        waves[2],
    )

    block = rows // shots
    part = jax.ShapeDtypeStruct((shots // 2, depth, block, cols), jnp.float32)
    splits = pl.pallas_call(
        split_kernel,
        out_shape=(part, part),
        in_specs=[SMEM] + [VMEM] * 3,
        out_specs=(VMEM, VMEM),
        compiler_params=params(10),
        cost_estimate=cost(2),
        name="split",
    )
    kept, sent = splits((shot % 2).reshape(1).astype(jnp.int32), image, last, waves[3])
    hop = 1
    while True:
        arrived = lax.ppermute(sent, "shot", [(i, i ^ hop) for i in range(shots)])
        hop *= 2
        if hop >= shots:
            break
        part = jax.ShapeDtypeStruct((kept.shape[0] // 2,) + kept.shape[1:], jnp.float32)
        kept, sent = pl.pallas_call(
            halve_kernel,
            out_shape=(part, part),
            in_specs=[SMEM] + [VMEM] * 2,
            out_specs=(VMEM, VMEM),
            compiler_params=params(8),
            cost_estimate=cost(1),
            name="halve",
        )(((shot // hop) % 2).reshape(1).astype(jnp.int32), kept, arrived)
    gradient = pl.pallas_call(
        add_kernel,
        out_shape=jax.ShapeDtypeStruct(kept.shape[1:], jnp.float32),
        in_specs=[VMEM] * 2,
        out_specs=VMEM,
        compiler_params=params(8),
        cost_estimate=cost(1),
        name="finish",
    )(kept[0], arrived[0])

    misfit = misfit_of(squares, 0.5 / (shots * ITERS * receivers * slabs)).reshape(())
    return (gradient, waves[4][None], waves[3][None], misfit)


def solution(mesh):
    placed = (
        P("shot", "space", None, None),
        P("shot", "space", None, None),
        P("space", None, None),
        P("shot", None, "space", None, None),
        P("shot", None, "space", None),
        P(),
        P("shot", "space"),
        P("shot", None, "space"),
        P("shot", None),
    )
    return jax.shard_map(
        body,
        mesh=mesh,
        in_specs=placed,
        out_specs=(
            P("space", "shot", None),
            P("shot", "space", None, None),
            P("shot", "space", None, None),
            P(),
        ),
        check_vma=False,
    )
```

```python
import functools

import jax
import jax.numpy as jnp
from jax import lax
from jax.experimental import pallas as pl
from jax.experimental.pallas import tpu as pltpu
from jax.sharding import PartitionSpec as P


ITERS = 4
MUTE = 8
LANES = 128
SUB = 8
REACH = 4
TAIL = 1

COEFFS = (-205.0 / 72.0, 8.0 / 5.0, -1.0 / 5.0, 8.0 / 315.0, -1.0 / 560.0)

VMEM = pl.BlockSpec(memory_space=pltpu.VMEM)
SMEM = pl.BlockSpec(memory_space=pltpu.SMEM)
HBM = pl.BlockSpec(memory_space=pltpu.HBM)


def params(mib):
    return pltpu.CompilerParams(vmem_limit_bytes=mib * 1024 * 1024)


def cost(us):
    return pl.CostEstimate(flops=int(us * 5e6), bytes_accessed=0, transcendentals=0)


def quotient(value, by):
    if by & (by - 1) == 0:
        return jnp.right_shift(value, by.bit_length() - 1)
    return value // by


def stack_planes(source, first, count, ypad):
    _, rows, cols = source.shape
    zero = jnp.zeros((SUB, LANES), jnp.float32)

    def step(j, carry):
        for t in range(cols // LANES):
            ypad[j, t, 0:SUB, :] = zero
            ypad[j, t, SUB + rows : 2 * SUB + rows, :] = zero
            ypad[j, t, SUB : SUB + rows, :] = source[first + j, :, t * LANES : (t + 1) * LANES]
        return carry

    lax.fori_loop(0, count, step, 0)


def update_planes(count, ypad, column, column_first, place, later, courant, added, new):
    _, rows, cols = new.shape
    tiles = cols // LANES
    lane = lax.broadcasted_iota(jnp.int32, (SUB, LANES), 1)
    zero = jnp.zeros((SUB, LANES), jnp.float32)

    def plane(j, carry):
        z = place + j
        for r in range(rows // SUB):
            y = slice(r * SUB, (r + 1) * SUB)
            centre = [ypad[j, t, SUB + r * SUB : 2 * SUB + r * SUB, :] for t in range(tiles)]
            total = [3.0 * COEFFS[0] * c for c in centre]
            for i in range(1, REACH + 1):
                right = [pltpu.roll(c, i, 1) for c in centre]
                left = [pltpu.roll(c, LANES - i, 1) for c in centre]
                for t in range(tiles):
                    x = slice(t * LANES, (t + 1) * LANES)
                    before = jnp.where(lane < i, right[t - 1] if t else zero, right[t])
                    after = jnp.where(
                        lane >= LANES - i, left[t + 1] if t + 1 < tiles else zero, left[t]
                    )
                    near = ypad[j, t, SUB + r * SUB - i : 2 * SUB + r * SUB - i, :]
                    far = ypad[j, t, SUB + r * SUB + i : 2 * SUB + r * SUB + i, :]
                    below = column[column_first + j - i, y, x]
                    above = column[column_first + j + i, y, x]
                    total[t] = total[t] + COEFFS[i] * (
                        ((before + after) + (near + far)) + (below + above)
                    )
            for t in range(tiles):
                x = slice(t * LANES, (t + 1) * LANES)
                value = (2.0 * centre[t] - later[z, y, x]) + (
                    courant[z, y, x] * total[t] + added[z, y, x]
                )
                new[j, y, x] = value
        return carry

    lax.fori_loop(0, count, plane, 0)


def inner_kernel(now, later, courant, added, new, ypad):
    depth = now.shape[0]
    count = depth - 2 * REACH
    stack_planes(now, REACH, count, ypad)
    update_planes(count, ypad, now, REACH, REACH, later, courant, added, new)


def edge_place(slab, paired, depth):
    even = lax.rem(slab[0], 2) == 0
    high, low = depth - REACH, 0
    return jnp.where(even, high, low) if paired else jnp.where(even, low, high)


def edge(first, now, halos, later, courant, added, strip, ypad, column):
    depth = now.shape[0]
    high = first > 0
    halo_at = jnp.where(high, 2 * REACH, 0)
    own_at = jnp.where(high, 0, REACH)
    own_first = jnp.where(high, depth - 2 * REACH, 0)
    at = 0
    for halo in halos:

        def copy_halo(j, carry, halo=halo, at=at):
            column[halo_at + at + j] = halo[j]
            return carry

        lax.fori_loop(0, halo.shape[0], copy_halo, 0)
        at += halo.shape[0]

    def copy_own(j, carry):
        column[own_at + j] = now[own_first + j]
        return carry

    lax.fori_loop(0, 2 * REACH, copy_own, 0)
    stack_planes(now, first, REACH, ypad)
    update_planes(REACH, ypad, column, REACH, first, later, courant, added, strip)


def cross_kernel(slab, now, halo, later, courant, added, strip, ypad, column):
    first = edge_place(slab, False, now.shape[0])
    edge(first, now, (halo,), later, courant, added, strip, ypad, column)


def pair_kernel(
    slab, now, lead, tail, later, courant, added, middle, other, new, sent, last, strip, ypad, column
):
    depth = now.shape[0]
    first = edge_place(slab, True, depth)
    edge(first, now, (lead, tail), later, courant, added, strip, ypad, column)
    opposite = depth - REACH - first
    cut = sent.shape[0]

    def copy_edges(j, carry):
        new[first + j] = strip[j]
        new[opposite + j] = other[j]
        return carry

    def copy_middle(j, carry):
        new[REACH + j] = middle[j]
        return carry

    def copy_sent(j, carry):
        sent[j] = strip[j]
        return carry

    def copy_last(j, carry):
        last[j] = strip[cut + j]
        return carry

    lax.fori_loop(0, REACH, copy_edges, 0)
    lax.fori_loop(0, depth - 2 * REACH, copy_middle, 0)
    lax.fori_loop(0, cut, copy_sent, 0)
    lax.fori_loop(0, REACH - cut, copy_last, 0)


def merge_kernel(slab, middle, other, out, sems):
    depth = out.shape[0]
    first = edge_place(slab, False, depth)
    copies = [
        pltpu.make_async_copy(part, out.at[pl.ds(at, part.shape[0])], sems.at[k])
        for k, (at, part) in enumerate(((REACH, middle), (first, other)))
    ]
    for copy in copies:
        copy.start()
    for copy in copies:
        copy.wait()


def store_kernel(value, out, sems):
    copy = pltpu.make_async_copy(value, out, sems.at[0])
    copy.start()
    copy.wait()


def last_kernel(
    slab, now, lead, tail, later, courant, added, partial, out, strip, ypad, column, sems
):
    del partial
    first = edge_place(slab, True, now.shape[0])
    edge(first, now, (lead, tail), later, courant, added, strip, ypad, column)
    copy = pltpu.make_async_copy(strip, out.at[pl.ds(first, REACH)], sems.at[0])
    copy.start()
    copy.wait()


def source_kernel(
    tiles, slab, cell, codes, index, table, observed, columns, squares, packed, onehot
):
    _, depth, rows, words = codes.shape
    cols = tiles * words
    count = cell.shape[1]
    flat = cell[...] - slab[0] * (depth * rows * cols)
    zy = quotient(flat, cols)
    x = flat - zy * cols
    z = quotient(zy, rows)
    block = (zy - z * rows) * tiles + quotient(x, LANES)
    packed[...] = jnp.zeros(packed.shape, jnp.float32)
    for k, line in enumerate((x, zy, z, block)):
        packed[k : k + 1, :] = line.astype(jnp.float32)
    packed[SUB : SUB + ITERS, :] = observed[...]
    turned = jnp.concatenate(
        [packed[:, k * LANES : (k + 1) * LANES].T for k in range(count // LANES)], axis=0
    )
    x_col, zy_col, z_col, block_col = (turned[:, k : k + 1].astype(jnp.int32) for k in range(4))
    one = jnp.ones((), jnp.float32)
    none = jnp.zeros((), jnp.float32)

    def hot(shape, col):
        return jnp.where(lax.broadcasted_iota(jnp.int32, shape, 1) == col, one, none)

    onehot[...] = hot((count, depth * rows), zy_col).astype(jnp.bfloat16)
    at_z = hot((count, depth), z_col).astype(jnp.bfloat16)
    at_x = lax.broadcasted_iota(jnp.int32, (count, cols), 1) == x_col
    at_block = lax.broadcasted_iota(jnp.int32, (count, rows * tiles), 1) == block_col
    total = jnp.zeros((count, 1), jnp.float32)
    columns[...] = jnp.zeros(columns.shape, jnp.float32)
    columns[:, ITERS : ITERS + 1] = turned[:, 0:1]
    for step in range(ITERS):
        level = ITERS - step
        word = codes[level].reshape(depth * rows, words)
        code = jnp.concatenate(
            [
                (jnp.bitwise_and(jnp.right_shift(word, 8 * m), 255) - 128)
                .astype(jnp.float32)
                .astype(jnp.bfloat16)
                for m in range(tiles)
            ],
            axis=1,
        )
        lines = jnp.dot(onehot[...], code, preferred_element_type=jnp.float32)
        picked = jnp.sum(jnp.where(at_x, lines, 0.0), axis=1, keepdims=True)
        entries = jnp.dot(
            at_z,
            index[level].astype(jnp.float32).astype(jnp.bfloat16),
            preferred_element_type=jnp.float32,
        )
        entry = jnp.sum(jnp.where(at_block, entries, 0.0), axis=1, keepdims=True)
        at_entry = lax.broadcasted_iota(jnp.int32, (count, table.shape[1]), 1) == entry.astype(
            jnp.int32
        )
        scale = jnp.sum(jnp.where(at_entry, table[...], 0.0), axis=1, keepdims=True)
        residual = picked * scale - turned[:, SUB + level - 1 : SUB + level]
        total = total + residual * residual
        columns[:, step : step + 1] = residual
    squares[...] = jnp.broadcast_to(jnp.sum(total, axis=0, keepdims=True), squares.shape)


def spread_kernel(step, slab, cell, columns, out, pieces):
    depth, rows, cols = out.shape
    count = cell.shape[1]
    zy = quotient(cell[...] - slab[0] * (depth * rows * cols), cols)
    lane = lax.broadcasted_iota(jnp.int32, (count, cols), 1)
    at_x = lane == columns[:, ITERS : ITERS + 1].astype(jnp.int32)
    dense = jnp.where(at_x, columns[:, step : step + 1], 0.0)
    for k in range(3):
        piece = dense.astype(jnp.bfloat16)
        pieces[k] = piece
        dense = dense - piece.astype(jnp.float32)
    one = jnp.ones((), jnp.float32)
    none = jnp.zeros((), jnp.float32)
    group = 4

    def planes(k, carry):
        rank = lax.broadcasted_iota(jnp.int32, (group * rows, count), 0) + k * (group * rows)
        at = jnp.where(rank == zy, one, none).astype(jnp.bfloat16)
        value = sum(jnp.dot(at, pieces[m], preferred_element_type=jnp.float32) for m in range(3))
        out[pl.ds(k * group, group)] = value.reshape(group, rows, cols)
        return carry

    lax.fori_loop(0, depth // group, planes, 0)


def image_kernel(
    slab, source, codes, index, table, w0, w1, w2, image, last, packed, turned, ey, held, field
):
    levels, depth, rows, _ = codes.shape
    cols = image.shape[2]
    tiles = cols // LANES
    first_z = slab[0] * depth
    source_z, source_y, source_x = (source[0, k] for k in range(3))
    scale_by = -1.0 / (2.0 * MUTE * MUTE)
    lane = lax.broadcasted_iota(jnp.int32, (SUB, LANES), 1)

    def bell(distance):
        off = distance.astype(jnp.float32)
        return jnp.exp(off * off * scale_by)

    packed[...] = jnp.zeros(packed.shape, jnp.float32)
    lines = levels * depth
    chosen = index[...].reshape(lines, rows * tiles)
    held[0:1, 0 : table.shape[1]] = table[...]
    across = jnp.broadcast_to(held[0:1, :], (lines, LANES))
    for h in range(rows * tiles // LANES):
        cut = slice(h * LANES, (h + 1) * LANES)
        packed[0:lines, cut] = jnp.take_along_axis(
            across, chosen[:, cut], axis=1, mode="promise_in_bounds"
        )
        turned[cut, :] = packed[:, cut].T
    ey[...] = bell(lax.broadcasted_iota(jnp.int32, (rows, LANES), 0) - source_y)
    ex = [bell(lane + (t * LANES) - source_x) for t in range(tiles)]

    def plane(z, carry):
        turn = lax.rem(LANES - z, LANES)
        for t in range(tiles):
            for r in range(rows // SUB):
                held[t * rows + r * SUB : t * rows + (r + 1) * SUB, :] = pltpu.roll(
                    turned[pl.ds(t + tiles * SUB * r, SUB, stride=tiles), :], turn, 1
                )
        for level in range(levels):
            lane_at = slice(level * depth, level * depth + 1)
            for r in range(rows // SUB):
                y = slice(r * SUB, (r + 1) * SUB)
                word = codes[level, z, y, :]
                for t in range(tiles):
                    at = slice(t * rows + r * SUB, t * rows + (r + 1) * SUB)
                    scale = jnp.broadcast_to(held[at, lane_at], (SUB, LANES))
                    code = jnp.bitwise_and(jnp.right_shift(word, 8 * t), 255) - 128
                    field[level, y, t * LANES : (t + 1) * LANES] = code.astype(jnp.float32) * scale
        ez = bell(jnp.full((SUB, LANES), first_z + z - source_z, jnp.int32))
        for r in range(rows // SUB):
            y = slice(r * SUB, (r + 1) * SUB)
            down = ez * ey[y, :]
            for t in range(tiles):
                x = slice(t * LANES, (t + 1) * LANES)
                value = [field[level, y, x] for level in range(levels)]
                bend = [
                    None if k in (0, levels - 1)
                    else (value[k + 1] - 2.0 * value[k]) + value[k - 1]
                    for k in range(levels)
                ]
                mute = 1.0 - down * ex[t]
                terms = w0[z, y, x] * bend[ITERS]
                terms = terms + w1[z, y, x] * bend[ITERS - 1]
                terms = terms + w2[z, y, x] * bend[ITERS - 2]
                image[z, y, x] = mute * terms
                last[z, y, x] = mute * bend[ITERS - 3]
        return carry

    lax.fori_loop(0, depth, plane, 0)


def cut_kernel(slab, shot, now, other, sent, last, sems):
    del shot
    depth = now.shape[0]
    cross = edge_place(slab, False, depth)
    pair = edge_place(slab, True, depth)
    cut = sent.shape[0]
    spans = ((cross, REACH, other), (pair, cut, sent), (pair + cut, REACH - cut, last))
    copies = [
        pltpu.make_async_copy(now.at[pl.ds(at, count)], out, sems.at[k])
        for k, (at, count, out) in enumerate(spans)
    ]
    for copy in copies:
        copy.start()
    for copy in copies:
        copy.wait()


def split_kernel(shot, image, last, w3, kept, sent):
    half, depth, block, _ = kept.shape
    mine = lax.rem(shot[0], 2)

    def plane(z, carry):
        for q in range(half):
            for out, which in ((kept, mine), (sent, 1 - mine)):
                y = pl.ds(pl.multiple_of((2 * q + which) * block, SUB), block)
                out[q, z] = image[z, y, :] + last[z, y, :] * w3[z, y, :]
        return carry

    lax.fori_loop(0, depth, plane, 0)


def halve_kernel(hop, shot, kept, arrived, keep, send):
    half, depth, _, _ = keep.shape
    mine = lax.rem(lax.div(shot[0], hop), 2)

    def plane(z, carry):
        for q in range(half):
            for out, which in ((keep, mine), (send, 1 - mine)):
                out[q, z] = kept[2 * q + which, z] + arrived[2 * q + which, z]
        return carry

    lax.fori_loop(0, depth, plane, 0)


def add_kernel(one, other, out):
    def plane(z, carry):
        out[z] = one[z] + other[z]
        return carry

    lax.fori_loop(0, out.shape[0], plane, 0)


def tile_add_kernel(one, other, out):
    out[...] = one[...] + other[...]


def scalar_kernel(factor, one, other, out):
    out[0, 0] = ((one[...] + other[...]) * factor)[0, 0]


def misfit_of(squares, factor):
    hops = []
    for axis, name in (("space", "m"), ("shot", "n")):
        count = lax.axis_size(axis)
        if count & (count - 1):
            squares = lax.psum(squares, axis)
            continue
        hop = 1
        while hop < count:
            hops.append((axis, f"{name}{hop}", [(i, i ^ hop) for i in range(count)]))
            hop *= 2
    for k, (axis, name, moves) in enumerate(hops):
        arrived = lax.ppermute(squares, axis, moves)
        last = k + 1 == len(hops)
        squares = pl.pallas_call(
            functools.partial(scalar_kernel, factor) if last else tile_add_kernel,
            out_shape=jax.ShapeDtypeStruct((1, 1) if last else squares.shape, jnp.float32),
            in_specs=[VMEM] * 2,
            out_specs=SMEM if last else VMEM,
            compiler_params=params(4),
            cost_estimate=cost(0.2),
            name="tally",
        )(squares, arrived)
    return squares


def body(
    adjoint_now,
    adjoint_later,
    courant,
    checkpoint_codes,
    scale_index,
    scale_table,
    receiver_cell,
    observed,
    source_cell,
):
    now = adjoint_now[0]
    later = adjoint_later[0]
    codes = checkpoint_codes[0]
    index = scale_index[0]
    depth, rows, cols = now.shape
    levels = codes.shape[0]
    tiles = cols // LANES
    receivers = receiver_cell.shape[1]
    slabs = lax.axis_size("space")
    shots = lax.axis_size("shot")
    slab = lax.axis_index("space").reshape(1)
    shot = lax.axis_index("shot").reshape(1)
    pairs = [(i, i ^ 1) for i in range(slabs) if i ^ 1 < slabs]
    crosses = [(i, i + 1) for i in range(1, slabs - 1, 2)]
    crosses = crosses + [(b, a) for a, b in crosses]
    field = jax.ShapeDtypeStruct((depth, rows, cols), jnp.float32)
    strip = jax.ShapeDtypeStruct((REACH, rows, cols), jnp.float32)
    lead = jax.ShapeDtypeStruct((REACH - TAIL, rows, cols), jnp.float32)
    tail = jax.ShapeDtypeStruct((TAIL, rows, cols), jnp.float32)

    def pair_exchange(block):
        return lax.ppermute(block, "space", pairs)

    def cross_exchange(block):
        return lax.ppermute(block, "space", crosses)

    ypad = (tiles, rows + 2 * SUB, LANES)
    middle = jax.ShapeDtypeStruct((depth - 2 * REACH, rows, cols), jnp.float32)
    edge_scratch = [
        pltpu.VMEM((REACH,) + ypad, jnp.float32),
        pltpu.VMEM((3 * REACH, rows, cols), jnp.float32),
    ]
    inner = pl.pallas_call(
        inner_kernel,
        out_shape=middle,
        in_specs=[VMEM] * 4,
        out_specs=VMEM,
        scratch_shapes=[pltpu.VMEM((depth - 2 * REACH,) + ypad, jnp.float32)],
        compiler_params=params(10),
        cost_estimate=cost(3),
        name="inner",
    )
    cross = pl.pallas_call(
        cross_kernel,
        out_shape=strip,
        in_specs=[SMEM] + [VMEM] * 5,
        out_specs=VMEM,
        scratch_shapes=edge_scratch,
        compiler_params=params(6),
        cost_estimate=cost(2),
        name="cross",
    )
    pair = pl.pallas_call(
        pair_kernel,
        out_shape=(field, lead, tail),
        in_specs=[SMEM] + [VMEM] * 8,
        out_specs=(VMEM, VMEM, VMEM),
        scratch_shapes=[pltpu.VMEM((REACH, rows, cols), jnp.float32)] + edge_scratch,
        compiler_params=params(8),
        cost_estimate=cost(2),
        name="pair",
    )

    def pair_exchange_both(sent, last):
        sent = pair_exchange(sent)
        last = pair_exchange(last)
        return sent, last

    cross_sent, *pair_sent = pl.pallas_call(
        cut_kernel,
        out_shape=(strip, lead, tail),
        in_specs=[SMEM, SMEM, HBM],
        out_specs=(VMEM, VMEM, VMEM),
        scratch_shapes=[pltpu.SemaphoreType.DMA((3,))],
        compiler_params=params(4),
        cost_estimate=cost(1),
        name="cut",
    )(slab, shot, now)
    cross_halo = cross_exchange(cross_sent)
    pair_halo = pair_exchange_both(*pair_sent)

    table = scale_table.reshape(1, scale_table.shape[0])
    sources = pl.pallas_call(
        functools.partial(source_kernel, tiles),
        out_shape=(
            jax.ShapeDtypeStruct((receivers, LANES), jnp.float32),
            jax.ShapeDtypeStruct((SUB, LANES), jnp.float32),
        ),
        in_specs=[SMEM] + [VMEM] * 5,
        out_specs=(VMEM, VMEM),
        scratch_shapes=[
            pltpu.VMEM((LANES, receivers), jnp.float32),
            pltpu.VMEM((receivers, depth * rows), jnp.bfloat16),
        ],
        compiler_params=params(12),
        cost_estimate=cost(5),
        name="sources",
    )
    columns, squares = sources(
        slab, receiver_cell, codes, index, table, observed[0]
    )

    def spread(step):
        return pl.pallas_call(
            functools.partial(spread_kernel, step),
            out_shape=field,
            in_specs=[SMEM] + [VMEM] * 2,
            out_specs=VMEM,
            scratch_shapes=[pltpu.VMEM((3, receivers, cols), jnp.bfloat16)],
            compiler_params=params(8),
            cost_estimate=cost(2),
            name="spread",
        )(slab, receiver_cell, columns)

    waves = [now]
    for step in range(ITERS):
        now = waves[-1]
        added = spread(step)
        within = inner(now, later, courant, added)
        cross_sent = cross(slab, now, cross_halo, later, courant, added)
        if step + 1 < ITERS:
            cross_halo = cross_exchange(cross_sent)
        if step + 1 == ITERS:
            break
        new, *pair_sent = pair(
            slab,
            now,
            *pair_halo,
            later,
            courant,
            added,
            within,
            cross_sent,
        )
        pair_halo = pair_exchange_both(*pair_sent)
        later = now
        waves.append(new)

    adjoint_first = pl.pallas_call(
        merge_kernel,
        out_shape=field,
        in_specs=[SMEM] + [VMEM] * 2,
        out_specs=HBM,
        scratch_shapes=[pltpu.SemaphoreType.DMA((2,))],
        compiler_params=params(6),
        cost_estimate=cost(1),
        name="merge",
    )(slab, within, cross_sent)
    adjoint_first = pl.pallas_call(
        last_kernel,
        out_shape=field,
        in_specs=[SMEM] + [VMEM] * 6 + [HBM],
        out_specs=HBM,
        input_output_aliases={7: 0},
        scratch_shapes=[pltpu.VMEM((REACH, rows, cols), jnp.float32)]
        + edge_scratch
        + [pltpu.SemaphoreType.DMA((1,))],
        compiler_params=params(8),
        cost_estimate=cost(2),
        name="last",
    )(slab, now, *pair_halo, later, courant, added, adjoint_first)
    adjoint_second = pl.pallas_call(
        store_kernel,
        out_shape=field,
        in_specs=[VMEM],
        out_specs=HBM,
        scratch_shapes=[pltpu.SemaphoreType.DMA((1,))],
        compiler_params=params(4),
        cost_estimate=cost(1),
        name="store",
    )(now)

    images = pl.pallas_call(
        image_kernel,
        out_shape=(field, field),
        in_specs=[SMEM] * 2 + [VMEM] * 6,
        out_specs=(VMEM, VMEM),
        scratch_shapes=[
            pltpu.VMEM((LANES, rows * tiles), jnp.float32),
            pltpu.VMEM((rows * tiles, LANES), jnp.float32),
            pltpu.VMEM((rows, LANES), jnp.float32),
            pltpu.VMEM((tiles * rows, LANES), jnp.float32),
            pltpu.VMEM((levels, rows, cols), jnp.float32),
        ],
        compiler_params=params(12),
        cost_estimate=cost(5),
        name="image",
    )
    image, last = images(
        slab,
        source_cell,
        codes,
        index,
        table,
        waves[0],
        waves[1],
        waves[2],
    )

    block = rows // shots
    part = jax.ShapeDtypeStruct((shots // 2, depth, block, cols), jnp.float32)
    splits = pl.pallas_call(
        split_kernel,
        out_shape=(part, part),
        in_specs=[SMEM] + [VMEM] * 3,
        out_specs=(VMEM, VMEM),
        compiler_params=params(10),
        cost_estimate=cost(2),
        name="split",
    )
    kept, sent = splits(shot, image, last, waves[3])
    hop = 1
    while True:
        arrived = lax.ppermute(sent, "shot", [(i, i ^ hop) for i in range(shots)])
        hop *= 2
        if hop >= shots:
            break
        part = jax.ShapeDtypeStruct((kept.shape[0] // 2,) + kept.shape[1:], jnp.float32)
        kept, sent = pl.pallas_call(
            functools.partial(halve_kernel, hop),
            out_shape=(part, part),
            in_specs=[SMEM] + [VMEM] * 2,
            out_specs=(VMEM, VMEM),
            compiler_params=params(8),
            cost_estimate=cost(1),
            name="halve",
        )(shot, kept, arrived)
    gradient = pl.pallas_call(
        add_kernel,
        out_shape=jax.ShapeDtypeStruct(kept.shape[1:], jnp.float32),
        in_specs=[VMEM] * 2,
        out_specs=VMEM,
        compiler_params=params(8),
        cost_estimate=cost(1),
        name="finish",
    )(kept[0], arrived[0])

    misfit = misfit_of(squares, 0.5 / (shots * ITERS * receivers * slabs)).reshape(())
    return (gradient, adjoint_first[None], adjoint_second[None], misfit)


def solution(mesh):
    placed = (
        P("shot", "space", None, None),
        P("shot", "space", None, None),
        P("space", None, None),
        P("shot", None, "space", None, None),
        P("shot", None, "space", None),
        P(),
        P("shot", "space"),
        P("shot", None, "space"),
        P("shot", None),
    )
    return jax.shard_map(
        body,
        mesh=mesh,
        in_specs=placed,
        out_specs=(
            P("space", "shot", None),
            P("shot", "space", None, None),
            P("shot", "space", None, None),
            P(),
        ),
        check_vma=False,
    )
```
